512 devices in a mesh: row: 64 (over z, x), col: 8 (over y, core).
Axes of the slice: x: 4, y: 4, z: 16, core: 2. Of those that a mesh axis runs over, the one named last changes fastest.
Arguments:
- gate_up: bfloat16 [4, 2, 14336, 4096], P(None, None, 'row', 'col'), may hold values from -0.09375 to 0.09375
- down_weight: bfloat16 [4, 4096, 14336], P(None, 'row', 'col'), may hold values from -0.046875 to 0.046875
- query_output: bfloat16 [4, 2, 4096, 4096], P(None, None, 'row', 'col'), may hold values from -0.09375 to 0.09375
- probe_gate: bfloat16 [4, 2, 16, 4096], P(None, None, None, 'col'), may hold values from -6 to 6
- probe_down: bfloat16 [4, 16, 14336], P(None, None, 'col'), may hold values from -6 to 6
- probe_query: bfloat16 [4, 2, 16, 4096], P(None, None, None, 'col'), may hold values from -6 to 6
Outputs:
- vector_gate: float32 [4, 2, 16, 4096], P(None, None, None, 'col')
- vector_down: float32 [4, 16, 14336], P(None, None, 'col')
- vector_query: float32 [4, 2, 16, 4096], P(None, None, None, 'col')
- sigma_gate: float32 [4, 2, 16], replicated
- sigma_down: float32 [4, 16], replicated
- sigma_query: float32 [4, 2, 16], replicated
The draws below stay inside these ranges and needn't reach their ends.
All inputs are finite; a program needn't handle non-finite values.
Results may differ from the reference program's by a relative error of at most 0.0033.
Values may be sent and summed in bfloat16 or wider, within the bound.
No kernel may reach another device: no remote copies, remote signals or barrier semaphores. Data moves between devices by JAX's collectives and lax.ppermute only.
A program may use at most 64 MiB of HBM per device.

```python
import jax
import jax.numpy as jnp
from jax import lax

D = 4096
FF = 14336
LAYERS = 4
ITERS = 2
PROBES = 16


def block_scale(own_key, shape, split, least, high):
    def one(dim, parts):
        steps = jax.random.uniform(jax.random.fold_in(jax.random.fold_in(own_key, 6), dim), (parts,), jnp.float32, least / len(split), high / len(split))
        return jnp.repeat(jnp.exp(steps), shape[dim] // parts).reshape((-1,) + (1,) * (len(shape) - dim - 1))

    factor_of = one(*split[0])
    for cut in split[1:]:
        factor_of = factor_of * one(*cut)
    return factor_of


def bell_draw(rng, extent, width, bound, split=(), held_as=jnp.bfloat16):
    array = jax.random.normal(rng, extent, jnp.float32) * width
    if len(split) > 0:
        array = block_scale(rng, extent, split, -0.22, 0.18) * array
    return jnp.clip(array, min=-bound, max=bound).astype(held_as)


def setup_inputs(seed: int = 0) -> dict:
    key_list = jax.random.split(jax.random.key(seed), 7)
    gate_up = bell_draw(key_list[0], (LAYERS, 2, FF, D), D ** -0.5, 0.09375, ((2, 64), (3, 8)))
    down_weight = bell_draw(key_list[1], (LAYERS, D, FF), FF ** -0.5, 0.046875, ((1, 64), (2, 8)))
    query_output = bell_draw(key_list[2], (LAYERS, 2, D, D), D ** -0.5, 0.09375, ((2, 64), (3, 8)))
    probe_gate = bell_draw(key_list[3], (LAYERS, 2, PROBES, D), 1.0, 6.0, ((3, 8),))
    probe_down = bell_draw(key_list[4], (LAYERS, PROBES, FF), 1.0, 6.0, ((2, 8),))
    probe_query = bell_draw(key_list[5], (LAYERS, 2, PROBES, D), 1.0, 6.0, ((3, 8),))
    return dict(gate_up=gate_up, down_weight=down_weight, query_output=query_output, probe_gate=probe_gate, probe_down=probe_down, probe_query=probe_query)


epsilon = 1e-06

def power_iterate(weight, probe):
    vector = probe
    right_vec = None
    right_total = None
    for turn in range(ITERS):
        left_raw = jnp.dot(vector, weight.T, preferred_element_type=jnp.float32)
        left_mean = lax.optimization_barrier(jnp.sum(left_raw * left_raw, axis=1, keepdims=True)) / weight.shape[0]
        left_vec = left_raw.astype(jnp.bfloat16)
        right_raw = jnp.dot(left_vec, weight, preferred_element_type=jnp.float32) * lax.rsqrt(left_mean + epsilon)
        right_total = lax.optimization_barrier(jnp.sum(right_raw * right_raw, axis=1, keepdims=True))
        right_vec = right_raw * lax.rsqrt(right_total / weight.shape[1] + epsilon)
        vector = right_vec.astype(jnp.bfloat16)
    spectral = jnp.sqrt(right_total[:, 0] / weight.shape[0])
    return (right_vec, spectral)

def reference(gate_up, down_weight, query_output, probe_gate, probe_down, probe_query):
    gate_vecs, gate_sig, down_vecs, down_sig, query_vecs, query_sig = ([], [], [], [], [], [])
    for layer in range(LAYERS):
        inner_v, inner_s = ([], [])
        for which in range(2):
            result_v, result_s = power_iterate(gate_up[layer, which], probe_gate[layer, which])
            inner_v.append(result_v)
            inner_s.append(result_s)
        gate_vecs.append(jnp.stack(inner_v))
        gate_sig.append(jnp.stack(inner_s))
        result_v, result_s = power_iterate(down_weight[layer], probe_down[layer])
        down_vecs.append(result_v)
        down_sig.append(result_s)
        inner_v, inner_s = ([], [])
        for which in range(2):
            result_v, result_s = power_iterate(query_output[layer, which], probe_query[layer, which])
            inner_v.append(result_v)
            inner_s.append(result_s)
        query_vecs.append(jnp.stack(inner_v))
        query_sig.append(jnp.stack(inner_s))
    return (jnp.stack(gate_vecs), jnp.stack(down_vecs), jnp.stack(query_vecs), jnp.stack(gate_sig), jnp.stack(down_sig), jnp.stack(query_sig))
```

```python
import functools

import jax
import jax.numpy as jnp
from jax import lax
from jax.experimental import pallas as pl
from jax.experimental.pallas import tpu as pltpu
from jax.sharding import Mesh
from jax.sharding import PartitionSpec as P

F32 = jnp.float32
BF16 = jnp.bfloat16
EPS = 1e-06
VMEM = pl.BlockSpec(memory_space=pltpu.VMEM)
LANES = 128


def call(kernel, outs, *args):
    return pl.pallas_call(
        kernel,
        out_shape=outs,
        in_specs=[VMEM] * len(args),
        out_specs=jax.tree.map(lambda _: VMEM, outs),
    )(*args)


def sds(shape, dtype):
    return jax.ShapeDtypeStruct(shape, dtype)


class Plan:
    def __init__(self, weights, xs, zs, cols):
        self.xs, self.zs, self.cols = xs, zs, cols
        self.rows = xs * zs
        self.outs = []
        self.ins = []
        self.where = []
        used = [0] * xs
        for w in weights:
            count, out, inp = w.shape
            per = count // xs
            for m in range(count):
                part = m // per
                self.where.append((part, used[part]))
                used[part] += inp // LANES
                self.outs.append(out)
                self.ins.append(inp)
        self.data = max(used)
        self.blocks = -(-(self.data + 2) // zs) * zs
        self.mine = self.blocks // zs
        self.left = []
        at = 0
        for out in self.outs:
            self.left.append(at)
            at += out
        self.left_end = at
        self.left_pad = -(-at // LANES) * LANES
        self.left_width = self.left_pad + LANES


def weight_of(refs, m):
    for ref in refs:
        if m < ref.shape[0]:
            return ref[m]
        m -= ref.shape[0]


def lane_table(columns, probes):
    lane = lax.broadcasted_iota(jnp.int32, (probes, LANES), 1)
    table = jnp.zeros((probes, LANES), F32)
    for m, column in enumerate(columns):
        table = jnp.where(lane == m, column, table)
    return table


def put_left(plan, lefts, table, out_ref):
    whole = jnp.concatenate(lefts, axis=1)
    pad = plan.left_pad - plan.left_end
    if pad:
        whole = jnp.concatenate([whole, jnp.zeros((whole.shape[0], pad), F32)], axis=1)
    for j in range(plan.cols):
        out_ref[j, :, : plan.left_pad] = whole
        out_ref[j, :, plan.left_pad :] = table


def dot_left(v, w):
    return lax.dot_general(v, w, (((1,), (1,)), ((), ())), preferred_element_type=F32)


def first_left(plan, a, b, c, va, vb, vc, out_ref):
    weights, probes = (a, b, c), (va, vb, vc)
    lefts = []
    for m in range(len(plan.outs)):
        lefts.append(dot_left(weight_of(probes, m), weight_of(weights, m)))
    put_left(plan, lefts, jnp.zeros((lefts[0].shape[0], LANES), F32), out_ref)


def vector_of(plan, v_ref, m, probes):
    part, first = plan.where[m]
    n = plan.ins[m] // LANES
    return jnp.concatenate(
        [v_ref[part, (first + k) * probes : (first + k + 1) * probes, :] for k in range(n)], axis=1
    )


def next_left(plan, a, b, c, v_ref, out_ref):
    weights = (a, b, c)
    probes = v_ref.shape[1] // plan.blocks
    lefts, squares = [], []
    for m in range(len(plan.outs)):
        v = vector_of(plan, v_ref, m, probes)
        wide = v.astype(F32)
        squares.append(jnp.sum(wide * wide, axis=1, keepdims=True))
        lefts.append(dot_left(v, weight_of(weights, m)))
    put_left(plan, lefts, lane_table(squares, probes), out_ref)


def right_body(plan, a, b, c, l_ref, out_ref):
    weights = (a, b, c)
    total = l_ref[0]
    for j in range(1, plan.cols):
        total = total + l_ref[j]
    probes = total.shape[0]
    squares = []
    for m in range(len(plan.outs)):
        raw = total[:, plan.left[m] : plan.left[m] + plan.outs[m]]
        squares.append(jnp.sum(raw * raw, axis=1, keepdims=True))
        right = jnp.dot(raw.astype(BF16), weight_of(weights, m), preferred_element_type=F32)
        part, first = plan.where[m]
        for k in range(plan.ins[m] // LANES):
            at = (first + k) * probes
            out_ref[part, at : at + probes, :] = right[:, k * LANES : (k + 1) * LANES]
    table = lane_table(squares, probes)
    zero = jnp.zeros((probes, LANES), F32)
    for x in range(plan.xs):
        for k in range(plan.data, plan.blocks):
            out_ref[x, k * probes : (k + 1) * probes, :] = table if k == plan.blocks - 2 else zero
    return total[:, plan.left_pad :]


def first_right(plan, a, b, c, l_ref, out_ref):
    right_body(plan, a, b, c, l_ref, out_ref)


def last_right(plan, a, b, c, l_ref, out_ref, q_ref):
    q_ref[...] = right_body(plan, a, b, c, l_ref, out_ref)


def sum_parts(in_ref, out_ref):
    total = in_ref[0]
    for j in range(1, in_ref.shape[0]):
        total = total + in_ref[j]
    out_ref[...] = total


def sum_copies(exact, probes, last_ref, in_ref, out_ref):
    total = in_ref[0]
    for j in range(1, in_ref.shape[0]):
        total = total + in_ref[j]
    if not exact:
        n = total.shape[0]
        high = total[n - 2 * probes : n - probes]
        low = high - high.astype(BF16).astype(F32)
        is_last = last_ref[...] > 0.5
        tail = jnp.where(is_last, low, total[n - probes :])
        total = jnp.concatenate([total[: n - probes], tail], axis=0).astype(BF16)
    for j in range(out_ref.shape[0]):
        out_ref[j] = total


def last_squares(plan, v_ref, out_ref):
    probes = v_ref.shape[1] // plan.blocks
    squares = []
    for m in range(len(plan.outs)):
        v = vector_of(plan, v_ref, m, probes)
        squares.append(jnp.sum(v * v, axis=1, keepdims=True))
    table = lane_table(squares, probes)
    for j in range(plan.cols):
        out_ref[j] = table


def finish(plan, v1_ref, q1_ref, v2_ref, q2_ref, oa, ob, oc, sigma_ref):
    probes = q1_ref.shape[0]
    lane = lax.broadcasted_iota(jnp.int32, (probes, LANES), 1)
    outs = jnp.zeros((probes, LANES), F32) + 1.0
    ins = outs
    for m in range(len(plan.outs)):
        outs = jnp.where(lane == m, float(plan.outs[m] * plan.rows), outs)
        ins = jnp.where(lane == m, float(plan.ins[m] * plan.cols), ins)
    n = plan.blocks * probes
    t1 = v1_ref[0, n - 2 * probes : n - probes, :].astype(F32) + v1_ref[0, n - probes :, :].astype(F32)
    f1 = lax.rsqrt(t1 / outs + EPS)
    s1 = f1 * lax.rsqrt(f1 * f1 * q1_ref[...] / ins + EPS)
    t2 = v2_ref[0, n - 2 * probes : n - probes, :]
    f2 = s1 * lax.rsqrt(s1 * s1 * t2 / outs + EPS)
    q2 = q2_ref[0]
    for j in range(1, plan.cols):
        q2 = q2 + q2_ref[j]
    total = f2 * f2 * q2
    scale = f2 * lax.rsqrt(total / ins + EPS)
    sigma_ref[...] = jnp.sqrt(total / outs)
    m = 0
    for ref in (oa, ob, oc):
        for k in range(ref.shape[0]):
            part, first = plan.where[m]
            for b in range(plan.ins[m] // LANES):
                at = (first + b) * probes
                ref[k, :, b * LANES : (b + 1) * LANES] = (
                    v2_ref[part, at : at + probes, :] * scale[:, m : m + 1]
                )
            m += 1


def swap(v, axis):
    return lax.all_to_all(v, axis, 0, 0, tiled=True)


def body(gate_up, down_weight, query_output, probe_gate, probe_down, probe_query):
    xs, zs, cols = lax.axis_size("x"), lax.axis_size("z"), lax.axis_size("col")
    flat = lambda w: w.reshape(-1, *w.shape[-2:])
    weights = tuple(flat(w) for w in (gate_up, down_weight, query_output))
    vectors = tuple(flat(v) for v in (probe_gate, probe_down, probe_query))
    probes = vectors[0].shape[1]
    plan = Plan(weights, xs, zs, cols)
    bind = lambda f, *rest: functools.partial(f, *rest)
    height = plan.blocks * probes
    mine = plan.mine * probes
    left_shape = sds((cols, probes, plan.left_width), F32)
    right_shape = sds((xs, height, LANES), F32)
    is_last = jnp.broadcast_to(
        (lax.axis_index("z") == zs - 1).astype(F32), (probes, LANES)
    )

    def reduce_row(right, exact):
        right = swap(right, "x")
        right = call(sum_parts, sds((height, LANES), F32), right)
        right = swap(right.reshape(zs, mine, LANES), "z")
        out = sds((zs, mine, LANES), F32 if exact else BF16)
        right = call(bind(sum_copies, exact, probes), out, is_last, right)
        right = swap(right, "z").reshape(1, height, LANES)
        return swap(jnp.broadcast_to(right, (xs, height, LANES)), "x")

    left = call(bind(first_left, plan), left_shape, *weights, *vectors)
    left = swap(left, "col")
    right = call(bind(first_right, plan), right_shape, *weights, left)
    v1 = reduce_row(right, False)
    left = call(bind(next_left, plan), left_shape, *weights, v1)
    left = swap(left, "col")
    right, q1 = call(
        bind(last_right, plan), (right_shape, sds((probes, LANES), F32)), *weights, left
    )
    v2 = reduce_row(right, True)
    q2 = call(bind(last_squares, plan), sds((cols, probes, LANES), F32), v2)
    q2 = swap(q2, "col")
    outs = tuple(sds(v.shape, F32) for v in vectors) + (sds((probes, LANES), F32),)
    oa, ob, oc, sigma = call(bind(finish, plan), outs, v1, q1, v2, q2)
    na, nb, nc = (w.shape[0] for w in weights)
    sigma = sigma.T
    sa, sb, sc = sigma[:na], sigma[na : na + nb], sigma[na + nb : na + nb + nc]
    like = lambda s, p: s.reshape(p.shape[:-1])
    return (
        oa.reshape(probe_gate.shape),
        ob.reshape(probe_down.shape),
        oc.reshape(probe_query.shape),
        like(sa, probe_gate),
        like(sb, probe_down),
        like(sc, probe_query),
    )


def solution(mesh):
    z = 16
    finer = Mesh(mesh.devices.reshape(z, -1, mesh.shape["col"]), ("z", "x", "col"))
    row = ("z", "x")
    in_specs = (
        P(None, None, row, "col"),
        P(None, row, "col"),
        P(None, None, row, "col"),
        P(None, None, None, "col"),
        P(None, None, "col"),
        P(None, None, None, "col"),
    )
    out_specs = (
        P(None, None, None, "col"),
        P(None, None, "col"),
        P(None, None, None, "col"),
        P(),
        P(),
        P(),
    )
    return jax.shard_map(body, mesh=finer, in_specs=in_specs, out_specs=out_specs, check_vma=False)
```

```python
import functools

import jax
import jax.numpy as jnp
from jax import lax
from jax.experimental import pallas as pl
from jax.experimental.pallas import tpu as pltpu
from jax.sharding import Mesh
from jax.sharding import PartitionSpec as P

F32 = jnp.float32
BF16 = jnp.bfloat16
EPS = 1e-06
VMEM = pl.BlockSpec(memory_space=pltpu.VMEM)
LANES = 128
LIMIT = 16 * 2**20
LEFT1, RIGHT1 = BF16, BF16
LEFT2, RIGHT2, GATHER2 = BF16, F32, BF16


def call(kernel, outs, *args):
    return pl.pallas_call(
        kernel,
        out_shape=outs,
        in_specs=[VMEM] * len(args),
        out_specs=jax.tree.map(lambda _: VMEM, outs),
        compiler_params=pltpu.CompilerParams(vmem_limit_bytes=LIMIT),
    )(*args)


def sds(shape, dtype):
    return jax.ShapeDtypeStruct(shape, dtype)


class Plan:
    def __init__(self, weights, xs, zs, cols):
        self.xs, self.zs, self.cols = xs, zs, cols
        self.rows = xs * zs
        self.outs = []
        self.ins = []
        self.where = []
        used = [0] * xs
        place = [0] * xs
        for w in weights:
            out, inp = w.shape[-2:]
            count = w.size // (out * inp)
            per = count // xs
            for m in range(count):
                part = m // per
                self.where.append((part, used[part], place[part]))
                used[part] += inp // LANES
                place[part] += 1
                self.outs.append(out)
                self.ins.append(inp)
        self.data = max(used)
        self.blocks = -(-(self.data + 2) // zs) * zs
        self.mine = self.blocks // zs
        self.left = []
        at = 0
        for out in self.outs:
            self.left.append(at)
            at += out
        self.left_end = at
        self.left_pad = -(-at // LANES) * LANES
        self.part = [
            (first, self.ins[m] // LANES)
            for m, (part, first, _) in enumerate(self.where)
            if part == 0
        ]


def matrix_of(refs, m):
    for ref in refs:
        n = ref.shape[0] * (ref.shape[1] if ref.ndim == 4 else 1)
        if m < n:
            return ref[m // ref.shape[1], m % ref.shape[1]] if ref.ndim == 4 else ref[m]
        m -= n


def lane_table(columns, probes):
    lane = lax.broadcasted_iota(jnp.int32, (probes, LANES), 1)
    table = jnp.zeros((probes, LANES), F32)
    for m, column in enumerate(columns):
        table = jnp.where(lane == m, column, table)
    return table


def pieces(table, dtype):
    high = table.astype(dtype)
    return high, (table - high.astype(F32)).astype(dtype)


def put_left(plan, lefts, table, out_ref):
    dtype = out_ref.dtype
    whole = jnp.concatenate(lefts, axis=1)
    pad = plan.left_pad - plan.left_end
    if pad:
        whole = jnp.concatenate([whole, jnp.zeros((whole.shape[0], pad), F32)], axis=1)
    whole = whole.astype(dtype)
    if table is not None:
        whole = jnp.concatenate([whole, *pieces(table, dtype)], axis=1)
    for j in range(plan.cols):
        out_ref[j] = whole


def dot_left(v, w):
    return lax.dot_general(v, w, (((1,), (1,)), ((), ())), preferred_element_type=F32)


def first_left(plan, a, b, c, va, vb, vc, out_ref):
    weights, probes = (a, b, c), (va, vb, vc)
    lefts = []
    for m in range(len(plan.outs)):
        lefts.append(dot_left(matrix_of(probes, m), matrix_of(weights, m)))
    put_left(plan, lefts, None, out_ref)


def vector_of(plan, v_ref, m, probes):
    part, first, _ = plan.where[m]
    n = plan.ins[m] // LANES
    return jnp.concatenate(
        [v_ref[part, (first + k) * probes : (first + k + 1) * probes, :] for k in range(n)], axis=1
    )


def next_left(plan, a, b, c, v_ref, out_ref):
    weights = (a, b, c)
    probes = v_ref.shape[1] // plan.blocks
    lefts, squares = [], []
    for m in range(len(plan.outs)):
        v = vector_of(plan, v_ref, m, probes)
        wide = v.astype(F32)
        squares.append(jnp.sum(wide * wide, axis=1, keepdims=True))
        lefts.append(dot_left(v, matrix_of(weights, m)))
    put_left(plan, lefts, lane_table(squares, probes), out_ref)


def sum_of(ref):
    total = ref[0].astype(F32)
    for j in range(1, ref.shape[0]):
        total = total + ref[j].astype(F32)
    return total


def right_body(plan, a, b, c, l_ref, out_ref, exact):
    weights = (a, b, c)
    total = sum_of(l_ref)
    probes = total.shape[0]
    dtype = out_ref.dtype
    squares = []
    for m in range(len(plan.outs)):
        raw = total[:, plan.left[m] : plan.left[m] + plan.outs[m]]
        squares.append(jnp.sum(raw * raw, axis=1, keepdims=True))
        weight = matrix_of(weights, m)
        high, low = pieces(raw, BF16)
        right = jnp.dot(high, weight, preferred_element_type=F32)
        if exact:
            right = right + jnp.dot(low, weight, preferred_element_type=F32)
        right = right.astype(dtype)
        part, first, _ = plan.where[m]
        for k in range(plan.ins[m] // LANES):
            at = (first + k) * probes
            out_ref[part, at : at + probes, :] = right[:, k * LANES : (k + 1) * LANES]
    high, low = pieces(lane_table(squares, probes), dtype)
    zero = jnp.zeros((probes, LANES), dtype)
    for x in range(plan.xs):
        for k in range(plan.data, plan.blocks):
            value = {plan.blocks - 2: high, plan.blocks - 1: low}.get(k, zero)
            out_ref[x, k * probes : (k + 1) * probes, :] = value
    return total


def first_right(plan, a, b, c, l_ref, out_ref):
    right_body(plan, a, b, c, l_ref, out_ref, False)


def last_right(plan, a, b, c, l_ref, out_ref, q_ref):
    total = right_body(plan, a, b, c, l_ref, out_ref, True)
    at = plan.left_pad
    q_ref[...] = total[:, at : at + LANES] + total[:, at + LANES :]


def tail_pieces(total, probes, dtype):
    n = total.shape[0]
    table = total[n - 2 * probes : n - probes] + total[n - probes :]
    return pieces(table, dtype)


def sum_parts(probes, in_ref, out_ref):
    total = sum_of(in_ref)
    n = total.shape[0]
    out_ref[...] = total.astype(out_ref.dtype)
    high, low = tail_pieces(total, probes, out_ref.dtype)
    out_ref[n - 2 * probes : n - probes, :] = high
    out_ref[n - probes :, :] = low


def sum_copies(probes, zs, in_ref, out_ref):
    total = sum_of(in_ref)
    n = total.shape[0]
    dtype = out_ref.dtype
    last = lax.axis_index("z") == zs - 1
    high, low = tail_pieces(total, probes, dtype)
    rounded = total.astype(dtype)
    for j in range(zs):
        out_ref[j] = rounded

    @pl.when(last)
    def _():
        for j in range(zs):
            out_ref[j, n - 2 * probes : n - probes, :] = high
            out_ref[j, n - probes :, :] = low


def part_squares(plan, v_ref, out_ref):
    probes = v_ref.shape[0] // plan.blocks
    columns = []
    for first, n in plan.part:
        total = jnp.zeros((probes, 1), F32)
        for k in range(first, first + n):
            v = v_ref[k * probes : (k + 1) * probes, :].astype(F32)
            total = total + jnp.sum(v * v, axis=1, keepdims=True)
        columns.append(total)
    table = lane_table(columns, probes)
    for j in range(out_ref.shape[0]):
        out_ref[j] = table


def finish(plan, v1_ref, q1_ref, v2_ref, q2_ref, oa, ob, oc, sa, sb, sc):
    probes = q1_ref.shape[0]
    lane = lax.broadcasted_iota(jnp.int32, (probes, LANES), 1)
    outs = jnp.zeros((probes, LANES), F32) + 1.0
    ins = outs
    for m in range(len(plan.outs)):
        outs = jnp.where(lane == m, float(plan.outs[m] * plan.rows), outs)
        ins = jnp.where(lane == m, float(plan.ins[m] * plan.cols), ins)
    n = plan.blocks * probes
    t1 = v1_ref[0, n - 2 * probes : n - probes, :].astype(F32) + v1_ref[0, n - probes :, :].astype(F32)
    f1 = lax.rsqrt(t1 / outs + EPS)
    s1 = f1 * lax.rsqrt(f1 * f1 * q1_ref[...] / ins + EPS)
    t2 = v2_ref[0, n - 2 * probes : n - probes, :].astype(F32) + v2_ref[0, n - probes :, :].astype(F32)
    f2 = s1 * lax.rsqrt(s1 * s1 * t2 / outs + EPS)
    by_part = []
    for x in range(plan.xs):
        q = q2_ref[x * plan.cols]
        for j in range(1, plan.cols):
            q = q + q2_ref[x * plan.cols + j]
        by_part.append(q)
    q2 = lane_table([by_part[part][:, i : i + 1] for part, _, i in plan.where], probes)
    total = f2 * f2 * q2
    scale = f2 * lax.rsqrt(total / ins + EPS)
    sigma = jnp.sqrt(total / outs).T
    m = 0
    for ref, sig in ((oa, sa), (ob, sb), (oc, sc)):
        n1, n2 = (ref.shape[0], 1) if ref.ndim == 3 else ref.shape[:2]
        if sig.ndim == 2:
            sig[...] = sigma[m : m + n1]
        else:
            for k in range(n1):
                sig[k] = sigma[m + k * n2 : m + (k + 1) * n2]
        for k in range(n1 * n2):
            part, first, _ = plan.where[m]
            for b in range(plan.ins[m] // LANES):
                at = (first + b) * probes
                value = v2_ref[part, at : at + probes, :].astype(F32) * scale[:, m : m + 1]
                here = slice(b * LANES, (b + 1) * LANES)
                if ref.ndim == 3:
                    ref[k, :, here] = value
                else:
                    ref[k // n2, k % n2, :, here] = value
            m += 1


def swap(v, axis):
    return lax.all_to_all(v, axis, 0, 0, tiled=True)


def body(gate_up, down_weight, query_output, probe_gate, probe_down, probe_query):
    xs, zs, cols = lax.axis_size("x"), lax.axis_size("z"), lax.axis_size("col")
    weights = (gate_up, down_weight, query_output)
    vectors = (probe_gate, probe_down, probe_query)
    probes = probe_down.shape[1]
    plan = Plan(weights, xs, zs, cols)
    bind = lambda f, *rest: functools.partial(f, *rest)
    height = plan.blocks * probes
    mine = plan.mine * probes

    def left_shape(extra, dtype):
        return sds((cols, probes, plan.left_pad + extra * LANES), dtype)

    def right_shape(dtype):
        return sds((xs, height, LANES), dtype)

    def reduce_row(right, gather):
        right = swap(right, "x")
        right = call(bind(sum_parts, probes), sds((height, LANES), right.dtype), right)
        right = swap(right.reshape(zs, mine, LANES), "z")
        right = call(bind(sum_copies, probes, zs), sds((zs, mine, LANES), gather), right)
        return swap(right, "z").reshape(height, LANES)

    def all_parts(right):
        return swap(jnp.broadcast_to(right[None], (xs, height, LANES)), "x")

    left = call(bind(first_left, plan), left_shape(0, LEFT1), *weights, *vectors)
    left = swap(left, "col")
    right = call(bind(first_right, plan), right_shape(RIGHT1), *weights, left)
    v1 = all_parts(reduce_row(right, BF16))
    left = call(bind(next_left, plan), left_shape(2, LEFT2), *weights, v1)
    left = swap(left, "col")
    right, q1 = call(
        bind(last_right, plan), (right_shape(RIGHT2), sds((probes, LANES), F32)), *weights, left
    )
    part = reduce_row(right, GATHER2)
    q2 = call(bind(part_squares, plan), sds((xs * cols, probes, LANES), F32), part)
    q2 = swap(q2, ("x", "col"))
    v2 = all_parts(part)
    outs = tuple(sds(v.shape, F32) for v in vectors)
    outs += tuple(sds(v.shape[:-1], F32) for v in vectors)
    return call(bind(finish, plan), outs, v1, q1, v2, q2)


def solution(mesh):
    z = 16
    finer = Mesh(mesh.devices.reshape(z, -1, mesh.shape["col"]), ("z", "x", "col"))
    row = ("z", "x")
    in_specs = (
        P(None, None, row, "col"),
        P(None, row, "col"),
        P(None, None, row, "col"),
        P(None, None, None, "col"),
        P(None, None, "col"),
        P(None, None, None, "col"),
    )
    out_specs = (
        P(None, None, None, "col"),
        P(None, None, "col"),
        P(None, None, None, "col"),
        P(),
        P(),
        P(),
    )
    return jax.shard_map(body, mesh=finer, in_specs=in_specs, out_specs=out_specs, check_vma=False)
```

```python
import functools

import jax
import jax.numpy as jnp
from jax import lax
from jax.experimental import pallas as pl
from jax.experimental.pallas import tpu as pltpu
from jax.sharding import Mesh
from jax.sharding import PartitionSpec as P

F32 = jnp.float32
BF16 = jnp.bfloat16
EPS = 1e-06
VMEM = pl.BlockSpec(memory_space=pltpu.VMEM)
LANES = 128
LIMIT = 16 * 2**20
WIRE = jnp.float16
TAIL = BF16
SECOND = 8
TOP = 2.0**15
HBM = pl.BlockSpec(memory_space=pltpu.HBM)


def call(kernel, outs, *args, specs=None, scratch=()):
    return pl.pallas_call(
        kernel,
        out_shape=outs,
        in_specs=specs or [VMEM] * len(args),
        out_specs=jax.tree.map(lambda _: VMEM, outs),
        scratch_shapes=scratch,
        compiler_params=pltpu.CompilerParams(vmem_limit_bytes=LIMIT),
    )(*args)


def sds(shape, dtype):
    return jax.ShapeDtypeStruct(shape, dtype)


class Plan:
    def __init__(self, weights, xs, zs, cols):
        self.xs, self.zs, self.cols = xs, zs, cols
        self.rows = xs * zs
        self.outs = []
        self.ins = []
        self.where = []
        used = [0] * xs
        place = [0] * xs
        for w in weights:
            out, inp = w.shape[-2:]
            count = w.size // (out * inp)
            per = count // xs
            for m in range(count):
                part = m // per
                self.where.append((part, used[part], place[part]))
                used[part] += inp // LANES
                place[part] += 1
                self.outs.append(out)
                self.ins.append(inp)
        self.data = max(used)
        assert max(place) <= SECOND
        self.blocks = self.data + 2 + (-(self.data + 2)) % 16
        self.high, self.low = self.blocks - 2, self.blocks - 1
        self.left = []
        at = 0
        for out in self.outs:
            self.left.append(at)
            at += out
        self.left_end = at
        self.left_pad = -(-at // LANES) * LANES
        self.part = [
            (first, self.ins[m] // LANES, self.ins[m])
            for m, (part, first, _) in enumerate(self.where)
            if part == 0
        ]

    def counts(self, probes):
        lane = lax.broadcasted_iota(jnp.int32, (probes, LANES), 1)
        outs = jnp.zeros((probes, LANES), F32) + 1.0
        ins = outs
        for m in range(len(self.outs)):
            outs = jnp.where(lane == m, float(self.outs[m] * self.rows), outs)
            ins = jnp.where(lane == m, float(self.ins[m] * self.cols), ins)
        return outs, ins


def matrix_of(refs, m):
    for ref in refs:
        n = ref.shape[0] * (ref.shape[1] if ref.ndim == 4 else 1)
        if m < n:
            return ref[m // ref.shape[1], m % ref.shape[1]] if ref.ndim == 4 else ref[m]
        m -= n


def lane_table(columns, rows, base=0):
    lane = lax.broadcasted_iota(jnp.int32, (rows, LANES), 1)
    table = jnp.zeros((rows, LANES), F32)
    for m, column in enumerate(columns):
        table = jnp.where(lane == m + base, column, table)
    return table


def pieces(table, dtype):
    high = table.astype(dtype)
    return high, (table - high.astype(F32)).astype(dtype)


def by_matrix(plan, parts, base=0):
    columns = [parts[part][:, base + i : base + i + 1] for part, _, i in plan.where]
    return lane_table(columns, parts[0].shape[0])


def put_left(plan, lefts, table, out_ref):
    dtype = out_ref.dtype
    whole = jnp.concatenate(lefts, axis=1)
    pad = plan.left_pad - plan.left_end
    if pad:
        whole = jnp.concatenate([whole, jnp.zeros((whole.shape[0], pad), F32)], axis=1)
    whole = jnp.concatenate([whole.astype(dtype), *pieces(table, dtype)], axis=1)
    for j in range(plan.cols):
        out_ref[j] = whole


def dot_left(v, w):
    return lax.dot_general(v, w, (((1,), (1,)), ((), ())), preferred_element_type=F32)


def first_left(plan, a, b, c, va, vb, vc, out_ref, *scratch):
    held, sems = scratch[:6], scratch[6]
    copies = []
    for k, (src, dst) in enumerate(zip((va, a, vb, b, vc, c), held)):
        copies.append(pltpu.make_async_copy(src, dst, sems.at[k]))
        copies[-1].start()
    lefts, norms = [], []
    for k in range(3):
        copies[2 * k].wait()
        copies[2 * k + 1].wait()
        probe, weight = held[2 * k], held[2 * k + 1]
        count = weight.shape[0] * (weight.shape[1] if weight.ndim == 4 else 1)
        for m in range(count):
            w = matrix_of((weight,), m)
            lefts.append(dot_left(matrix_of((probe,), m), w))
            wide = w.astype(F32)
            norms.append(jnp.sum(jnp.sum(wide * wide, axis=0, keepdims=True), axis=1, keepdims=True))
    put_left(plan, lefts, lane_table(norms, lefts[0].shape[0]), out_ref)


def vector_of(plan, v_ref, m):
    part, first, _ = plan.where[m]
    n = plan.ins[m] // LANES
    return jnp.concatenate([v_ref[part, first + k] for k in range(n)], axis=1)


def next_left(plan, a, b, c, v_ref, out_ref):
    weights = (a, b, c)
    probes = v_ref.shape[2]
    lefts, squares = [], []
    for m in range(len(plan.outs)):
        v = vector_of(plan, v_ref, m)
        wide = v.astype(F32)
        squares.append(jnp.sum(wide * wide, axis=1, keepdims=True))
        lefts.append(dot_left(v, matrix_of(weights, m)))
    put_left(plan, lefts, lane_table(squares, probes), out_ref)


def sum_of(ref):
    total = ref[0].astype(F32)
    for j in range(1, ref.shape[0]):
        total = total + ref[j].astype(F32)
    return total


def sum_left(plan, l_ref):
    total = sum_of(l_ref)
    at = plan.left_pad
    return total, total[:, at : at + LANES] + total[:, at + LANES :]


def put_right(plan, weights, total, scale, tables, out_ref, rows_ref):
    probes = total.shape[0]
    for m in range(len(plan.outs)):
        raw = total[:, plan.left[m] : plan.left[m] + plan.outs[m]]
        if scale is not None:
            raw = raw * scale[:, m : m + 1]
        weight = matrix_of(weights, m)
        high, low = pieces(raw, BF16)
        right = jnp.dot(high, weight, preferred_element_type=F32)
        right = right + jnp.dot(low, weight, preferred_element_type=F32)
        part, first, _ = plan.where[m]
        for k in range(plan.ins[m] // LANES):
            rows_ref[part, :, first + k, :] = right[:, k * LANES : (k + 1) * LANES]
    zero = jnp.zeros((probes, LANES), F32)
    for x in range(plan.xs):
        for k in range(plan.data, plan.high):
            rows_ref[x, :, k, :] = zero
        high = tables[x].astype(TAIL).astype(F32)
        rows_ref[x, :, plan.high, :] = high
        rows_ref[x, :, plan.low, :] = tables[x] - high
    if out_ref is not None:
        for x in range(plan.xs):
            out_ref[x] = rows_ref[x].astype(out_ref.dtype)


def left_squares(plan, total):
    squares = []
    for m in range(len(plan.outs)):
        raw = total[:, plan.left[m] : plan.left[m] + plan.outs[m]]
        squares.append(jnp.sum(raw * raw, axis=1, keepdims=True))
    return squares


def of_part(plan, x, columns):
    return [column for column, where in zip(columns, plan.where) if where[0] == x]


def first_right(plan, a, b, c, l_ref, out_ref, rows_ref):
    total, norms = sum_left(plan, l_ref)
    probes = total.shape[0]
    squares = left_squares(plan, total)
    norms = [norms[:, m : m + 1] for m in range(len(plan.outs))]
    tables = [
        lane_table(of_part(plan, x, squares), probes)
        + lane_table(of_part(plan, x, norms), probes, SECOND)
        for x in range(plan.xs)
    ]
    put_right(plan, (a, b, c), total, None, tables, out_ref, rows_ref)


def last_right(plan, a, b, c, l_ref, v_ref, out_ref, stats_ref):
    total, q1 = sum_left(plan, l_ref)
    probes = total.shape[0]
    outs, ins = plan.counts(probes)
    parts = [v_ref[x, plan.high].astype(F32) + v_ref[x, plan.low].astype(F32) for x in range(plan.xs)]
    t1 = by_matrix(plan, parts)
    norm = by_matrix(plan, parts, SECOND) * 1.01
    f1 = lax.rsqrt(t1 / outs + EPS)
    s1 = f1 * lax.rsqrt(f1 * f1 * q1 / ins + EPS)
    root = jnp.sqrt(q1 * 1.01 + 1e-33)
    scale = TOP / jnp.maximum(norm * root, 1e-30)
    square_scale = TOP / jnp.maximum(norm * root * root, 1e-30)
    stats_ref[0] = s1
    stats_ref[1] = scale
    stats_ref[2] = square_scale
    squares = [
        column * square_scale[:, m : m + 1] for m, column in enumerate(left_squares(plan, total))
    ]
    tables = [lane_table(of_part(plan, x, squares), probes) for x in range(plan.xs)]
    put_right(plan, (a, b, c), total, scale, tables, None, out_ref)


def split_again(plan, total, axis, dtype):
    row = lax.broadcasted_iota(jnp.int32, total.shape, axis)
    table = lax.slice_in_dim(total, plan.high, plan.high + 1, axis=axis)
    table = table + lax.slice_in_dim(total, plan.low, plan.low + 1, axis=axis)
    high = table.astype(dtype).astype(F32)
    return jnp.where(row == plan.high, high, jnp.where(row == plan.low, table - high, total))


def sum_parts(plan, in_ref, out_ref):
    dtype = out_ref.dtype
    out_ref[...] = split_again(plan, sum_of(in_ref), 1, dtype).astype(dtype)


def sum_copies(plan, in_ref, out_ref):
    dtype = out_ref.dtype
    total = split_again(plan, sum_of(in_ref), 0, dtype).astype(dtype)
    for j in range(plan.zs):
        out_ref[j] = total


def own_squares(plan, y_ref, out_ref):
    columns = []
    for first, n, _ in plan.part:
        y = y_ref[first : first + n, :]
        total = jnp.sum(y * y, axis=1, keepdims=True)
        columns.append(jnp.sum(total, axis=0, keepdims=True))
    table = lane_table(columns, out_ref.shape[1])
    for j in range(plan.cols):
        out_ref[j] = table


def unit(plan, y_ref, q_ref, out_ref):
    q = sum_of(q_ref)[:1]
    out_ref[...] = jnp.zeros(out_ref.shape, F32)
    for i, (first, n, inp) in enumerate(plan.part):
        factor = lax.rsqrt(jnp.maximum(q[:, i : i + 1] / float(inp * plan.cols), 1e-30))
        out_ref[first : first + n, :] = y_ref[first : first + n, :] * factor
    lane = lax.broadcasted_iota(jnp.int32, (1, LANES), 1)
    left = y_ref[plan.high : plan.high + 1, :] + y_ref[plan.low : plan.low + 1, :]
    left = [left[:, i : i + 1] for i in range(len(plan.part))]
    table = jnp.where(lane < SECOND, jnp.sqrt(q), lane_table(left, 1, SECOND))
    high = table.astype(TAIL).astype(F32)
    out_ref[plan.high : plan.high + 1, :] = high
    out_ref[plan.low : plan.low + 1, :] = table - high


def finish(plan, stats_ref, v_ref, oa, ob, oc, sa, sb, sc):
    probes = v_ref.shape[2]
    outs, ins = plan.counts(probes)
    parts = [v_ref[x, plan.high].astype(F32) + v_ref[x, plan.low].astype(F32) for x in range(plan.xs)]
    root = by_matrix(plan, parts)
    t2 = by_matrix(plan, parts, SECOND) / stats_ref[2]
    s1 = stats_ref[0]
    f2 = s1 * lax.rsqrt(s1 * s1 * t2 / outs + EPS)
    root = root / stats_ref[1] * f2
    spread = root * lax.rsqrt(ins)
    scale = spread * lax.rsqrt(spread * spread + EPS)
    sigma = (root * lax.rsqrt(outs)).T
    m = 0
    for ref, sig in ((oa, sa), (ob, sb), (oc, sc)):
        n1, n2 = (ref.shape[0], 1) if ref.ndim == 3 else ref.shape[:2]
        if sig.ndim == 2:
            sig[...] = sigma[m : m + n1]
        else:
            for k in range(n1):
                sig[k] = sigma[m + k * n2 : m + (k + 1) * n2]
        for k in range(n1 * n2):
            part, first, _ = plan.where[m]
            for b in range(plan.ins[m] // LANES):
                value = v_ref[part, first + b].astype(F32) * scale[:, m : m + 1]
                here = slice(b * LANES, (b + 1) * LANES)
                if ref.ndim == 3:
                    ref[k, :, here] = value
                else:
                    ref[k // n2, k % n2, :, here] = value
            m += 1


def swap(v, axis):
    return lax.all_to_all(v, axis, 0, 0, tiled=True)


def body(gate_up, down_weight, query_output, probe_gate, probe_down, probe_query):
    xs, zs, cols = lax.axis_size("x"), lax.axis_size("z"), lax.axis_size("col")
    weights = (gate_up, down_weight, query_output)
    vectors = (probe_gate, probe_down, probe_query)
    probes = probe_down.shape[1]
    plan = Plan(weights, xs, zs, cols)
    bind = lambda f, *rest: functools.partial(f, *rest)
    blocks = plan.blocks
    left_shape = sds((cols, probes, plan.left_pad + 2 * LANES), BF16)
    rows = pltpu.VMEM((xs, probes, blocks, LANES), F32)

    def right_shape(dtype):
        return sds((xs, probes, blocks, LANES), dtype)

    def gather(copies):
        part = jnp.swapaxes(swap(copies, "z"), 0, 1)
        return swap(jnp.broadcast_to(part[None], (xs, *part.shape)), "x")

    held = [pltpu.VMEM(x.shape, x.dtype) for pair in zip(vectors, weights) for x in pair]
    left = call(
        bind(first_left, plan),
        left_shape,
        *weights,
        *vectors,
        specs=[HBM] * 6,
        scratch=[*held, pltpu.SemaphoreType.DMA((6,))],
    )
    left = swap(left, "col")
    right = call(bind(first_right, plan), right_shape(BF16), *weights, left, scratch=[rows])
    right = swap(right, "x")
    right = call(bind(sum_parts, plan), sds((probes, blocks, LANES), BF16), right)
    right = swap(right, "z")
    v1 = gather(call(bind(sum_copies, plan), sds((zs, blocks, LANES), BF16), right))

    left = call(bind(next_left, plan), left_shape, *weights, v1)
    left = swap(left, "col")
    shapes = (right_shape(F32), sds((3, probes, LANES), F32))
    right, stats = call(bind(last_right, plan), shapes, *weights, left, v1)
    right = swap(right.astype(WIRE), "x")
    right = jnp.sum(right.astype(F32), axis=0).astype(WIRE)
    right = jnp.sum(swap(right, "z").astype(F32), axis=0)
    q2 = call(bind(own_squares, plan), sds((cols, 8, LANES), F32), right)
    q2 = swap(q2, "col")
    own = call(bind(unit, plan), sds((blocks, LANES), F32), right, q2)
    v2 = gather(jnp.broadcast_to(own.astype(WIRE)[None], (zs, *own.shape))).astype(F32)
    outs = tuple(sds(v.shape, F32) for v in vectors)
    outs += tuple(sds(v.shape[:-1], F32) for v in vectors)
    return call(bind(finish, plan), outs, stats, v2)


def solution(mesh):
    z = 16
    finer = Mesh(mesh.devices.reshape(z, -1, mesh.shape["col"]), ("z", "x", "col"))
    row = ("z", "x")
    in_specs = (
        P(None, None, row, "col"),
        P(None, row, "col"),
        P(None, None, row, "col"),
        P(None, None, None, "col"),
        P(None, None, "col"),
        P(None, None, None, "col"),
    )
    out_specs = (
        P(None, None, None, "col"),
        P(None, None, "col"),
        P(None, None, None, "col"),
        P(),
        P(),
        P(),
    )
    return jax.shard_map(body, mesh=finer, in_specs=in_specs, out_specs=out_specs, check_vma=False)
```

```python
import functools

import jax
import jax.numpy as jnp
from jax import lax
from jax.experimental import pallas as pl
from jax.experimental.pallas import tpu as pltpu
from jax.sharding import Mesh
from jax.sharding import PartitionSpec as P


F32 = jnp.float32
BF16 = jnp.bfloat16
EPS = 1e-06
VMEM = pl.BlockSpec(memory_space=pltpu.VMEM)
LANES = 128
LIMIT = 16 * 2**20
WIRE = jnp.float16
TAIL = BF16
COL = ("y", "core")
FIRST = 64 * 2**20 - 2**16 - 800 * 2**10
SECOND = 8
TOP = 2.0**15
HBM = pl.BlockSpec(memory_space=pltpu.HBM)


def call(kernel, outs, *args, specs=None, out_specs=None, scratch=(), limit=LIMIT):
    return pl.pallas_call(
        kernel,
        out_shape=outs,
        in_specs=specs or [VMEM] * len(args),
        out_specs=out_specs or jax.tree.map(lambda _: VMEM, outs),
        scratch_shapes=scratch,
        compiler_params=pltpu.CompilerParams(vmem_limit_bytes=limit),
    )(*args)


def sds(shape, dtype):
    return jax.ShapeDtypeStruct(shape, dtype)


class Plan:
    def __init__(self, weights, xs, zs, cols):
        self.xs, self.zs, self.cols = xs, zs, cols
        self.rows = xs * zs
        self.outs = []
        self.ins = []
        self.where = []
        used = [0] * xs
        place = [0] * xs
        for w in weights:
            out, inp = w.shape[-2:]
            count = w.size // (out * inp)
            per = count // xs
            for m in range(count):
                part = m // per
                self.where.append((part, used[part], place[part]))
                used[part] += inp // LANES
                place[part] += 1
                self.outs.append(out)
                self.ins.append(inp)
        self.data = max(used)
        assert max(place) <= SECOND
        self.blocks = self.data + 2 + (-(self.data + 2)) % 16
        self.high, self.low = self.blocks - 2, self.blocks - 1
        self.left = []
        at = 0
        for out in self.outs:
            self.left.append(at)
            at += out
        self.left_end = at
        self.left_pad = -(-at // LANES) * LANES
        self.part = [
            (first, self.ins[m] // LANES, self.ins[m])
            for m, (part, first, _) in enumerate(self.where)
            if part == 0
        ]

        self.places = []
        for f, w in enumerate(weights):
            assert w.shape[0] == xs
            for k in range(w.shape[1]) if w.ndim == 4 else (None,):
                self.places.append((f, k, w.shape[-2]))
        self.width = min(w.shape[-1] for w in weights)
        self.strips = []
        row = 0
        for (_, _, out), (_, _, inp) in zip(self.places, self.part):
            strips = []
            for lane in range(0, inp, self.width):
                strips.append((lane, min(self.width, inp - lane), row, out))
                row += out
            self.strips.append(strips)
        self.packed = row
        self.part_at = []
        at = 0
        for _, _, out in self.places:
            self.part_at.append(at)
            at += out
        self.part_rows = at

    def part_counts(self, probes):
        lane = lax.broadcasted_iota(jnp.int32, (probes, LANES), 1)
        outs = jnp.zeros((probes, LANES), F32) + 1.0
        ins = outs
        for i, (_, _, out) in enumerate(self.places):
            outs = jnp.where(lane == i, float(out * self.rows), outs)
            ins = jnp.where(lane == i, float(self.part[i][2] * self.cols), ins)
        return outs, ins

    def counts(self, probes):
        lane = lax.broadcasted_iota(jnp.int32, (probes, LANES), 1)
        outs = jnp.zeros((probes, LANES), F32) + 1.0
        ins = outs
        for m in range(len(self.outs)):
            outs = jnp.where(lane == m, float(self.outs[m] * self.rows), outs)
            ins = jnp.where(lane == m, float(self.ins[m] * self.cols), ins)
        return outs, ins


def matrix_of(refs, m):
    for ref in refs:
        n = ref.shape[0] * (ref.shape[1] if ref.ndim == 4 else 1)
        if m < n:
            return ref[m // ref.shape[1], m % ref.shape[1]] if ref.ndim == 4 else ref[m]
        m -= n


def lane_table(columns, rows, base=0):
    lane = lax.broadcasted_iota(jnp.int32, (rows, LANES), 1)
    table = jnp.zeros((rows, LANES), F32)
    for m, column in enumerate(columns):
        table = jnp.where(lane == m + base, column, table)
    return table


def pieces(table, dtype):
    high = table.astype(dtype)
    return high, (table - high.astype(F32)).astype(dtype)


def by_matrix(plan, parts, base=0):
    columns = [parts[part][:, base + i : base + i + 1] for part, _, i in plan.where]
    return lane_table(columns, parts[0].shape[0])


def join_left(plan, lefts, table):
    whole = jnp.concatenate(lefts, axis=1)
    pad = plan.left_pad - plan.left_end
    if pad:
        whole = jnp.concatenate([whole, jnp.zeros((whole.shape[0], pad), F32)], axis=1)
    return jnp.concatenate([whole, table], axis=1)


def put_copies(plan, total, out_ref):
    whole = total[:, : plan.left_pad].astype(BF16)
    whole = jnp.concatenate([whole, *pieces(total[:, plan.left_pad :], BF16)], axis=1)
    for j in range(out_ref.shape[0]):
        out_ref[j] = whole


def pair_sum(plan, mine_ref, other_ref, out_ref):
    put_copies(plan, mine_ref[...] + other_ref[...], out_ref)


def dot_left(v, w):
    return lax.dot_general(v, w, (((1,), (1,)), ((), ())), preferred_element_type=F32)


def first_left(plan, a, b, c, va, vb, vc, *refs):
    out_ref, packs = refs[0], refs[1 : 1 + plan.xs]
    *held, sems, pack_sems = refs[1 + plan.xs :]
    copies = []
    for k, (src, dst) in enumerate(zip((va, a, vb, b, vc, c), held)):
        copies.append(pltpu.make_async_copy(src, dst, sems.at[k]))
        copies[-1].start()
    me = lax.axis_index("x")
    moves = []

    def move(family, s):
        part = lax.rem(me + s, plan.xs)
        for i, (own, k, _) in enumerate(plan.places):
            if own != family:
                continue
            ref = held[2 * family + 1]
            src = ref.at[part] if k is None else ref.at[part, k]
            for lane, lanes, row, height in plan.strips[i]:
                moves.append(
                    pltpu.make_async_copy(
                        src.at[:, lane : lane + lanes],
                        packs[s].at[row : row + height, :lanes],
                        pack_sems.at[len(moves)],
                    )
                )
                moves[-1].start()

    lefts, norms = [], []
    for k in range(3):
        copies[2 * k].wait()
        copies[2 * k + 1].wait()
        for s in range(plan.xs):
            move(k, s)
        probe, weight = held[2 * k], held[2 * k + 1]
        count = weight.shape[0] * (weight.shape[1] if weight.ndim == 4 else 1)
        for m in range(count):
            w = matrix_of((weight,), m)
            lefts.append(dot_left(matrix_of((probe,), m), w))
            wide = w.astype(F32)
            norms.append(jnp.sum(jnp.sum(wide * wide, axis=0, keepdims=True), axis=1, keepdims=True))
    put_copies(plan, join_left(plan, lefts, lane_table(norms, lefts[0].shape[0])), out_ref)
    for copy in moves:
        copy.wait()


def next_left(plan, *refs):
    weights, v_ref, out_ref = refs[: plan.xs], refs[-2], refs[-1]
    vectors, squares = [], []
    for first, n, _ in plan.part:
        v = jnp.concatenate([v_ref[first + k] for k in range(n)], axis=1)
        wide = v.astype(F32)
        squares.append(jnp.sum(wide * wide, axis=1, keepdims=True))
        vectors.append(v)
    lefts = []
    for weight in weights:
        for v, strips in zip(vectors, plan.strips):
            left = 0.0
            for lane, lanes, row, height in strips:
                w = weight[row : row + height, :lanes]
                left = left + dot_left(v[:, lane : lane + lanes], w)
            lefts.append(left)
    out_ref[...] = join_left(plan, lefts, lane_table(squares, v_ref.shape[1]))


def sum_of(ref):
    total = ref[0].astype(F32)
    for j in range(1, ref.shape[0]):
        total = total + ref[j].astype(F32)
    return total


def sum_left(plan, l_ref):
    total = sum_of(l_ref)
    at = plan.left_pad
    return total, total[:, at : at + LANES] + total[:, at + LANES :]


def put_right(plan, weights, total, scale, tables, out_ref, rows_ref):
    probes = total.shape[0]
    for m in range(len(plan.outs)):
        raw = total[:, plan.left[m] : plan.left[m] + plan.outs[m]]
        if scale is not None:
            raw = raw * scale[:, m : m + 1]
        weight = matrix_of(weights, m)
        high, low = pieces(raw, BF16)
        right = jnp.dot(high, weight, preferred_element_type=F32)
        right = right + jnp.dot(low, weight, preferred_element_type=F32)
        part, first, _ = plan.where[m]
        for k in range(plan.ins[m] // LANES):
            rows_ref[part, :, first + k, :] = right[:, k * LANES : (k + 1) * LANES]
    zero = jnp.zeros((probes, LANES), F32)
    for x in range(plan.xs):
        for k in range(plan.data, plan.high):
            rows_ref[x, :, k, :] = zero
        high = tables[x].astype(TAIL).astype(F32)
        rows_ref[x, :, plan.high, :] = high
        rows_ref[x, :, plan.low, :] = tables[x] - high
    if out_ref is not None:
        for x in range(plan.xs):
            out_ref[x] = rows_ref[x].astype(out_ref.dtype)


def left_squares(plan, total):
    squares = []
    for m in range(len(plan.outs)):
        raw = total[:, plan.left[m] : plan.left[m] + plan.outs[m]]
        squares.append(jnp.sum(raw * raw, axis=1, keepdims=True))
    return squares


def of_part(plan, x, columns):
    return [column for column, where in zip(columns, plan.where) if where[0] == x]


def first_right(plan, a, b, c, l_ref, out_ref, rows_ref):
    total, norms = sum_left(plan, l_ref)
    probes = total.shape[0]
    squares = left_squares(plan, total)
    norms = [norms[:, m : m + 1] for m in range(len(plan.outs))]
    tables = [
        lane_table(of_part(plan, x, squares), probes)
        + lane_table(of_part(plan, x, norms), probes, SECOND)
        for x in range(plan.xs)
    ]
    put_right(plan, (a, b, c), total, None, tables, out_ref, rows_ref)


def last_right(plan, *refs):
    weights = refs[: plan.xs]
    l_ref, v_ref, rows_ref, stats_ref = refs[plan.xs :]
    total, q1 = sum_left(plan, l_ref)
    probes = total.shape[0]
    outs, ins = plan.part_counts(probes)
    tail = v_ref[plan.high].astype(F32) + v_ref[plan.low].astype(F32)
    here = range(len(plan.part))
    t1 = tail
    norm = lane_table([tail[:, SECOND + i : SECOND + i + 1] for i in here], probes) * 1.01
    f1 = lax.rsqrt(t1 / outs + EPS)
    s1 = f1 * lax.rsqrt(f1 * f1 * q1 / ins + EPS)
    root = jnp.sqrt(q1 * 1.01 + 1e-33)
    scale = TOP / jnp.maximum(norm * root, 1e-30)
    square_scale = TOP / jnp.maximum(norm * root * root, 1e-30)
    stats_ref[0] = s1
    stats_ref[1] = scale
    stats_ref[2] = square_scale
    squares = []
    for i in here:
        first, _, _ = plan.part[i]
        square = 0.0
        high, low = [], []
        for s in range(plan.xs):
            at = s * plan.part_rows + plan.part_at[i]
            raw = total[:, at : at + plan.places[i][2]]
            square = square + jnp.sum(raw * raw, axis=1, keepdims=True)
            both = pieces(raw * scale[:, i : i + 1], BF16)
            high.append(both[0])
            low.append(both[1])
        squares.append(square * square_scale[:, i : i + 1])
        for lane, lanes, row, height in plan.strips[i]:
            right = 0.0
            for s in range(plan.xs):
                w = weights[s][row : row + height, :lanes]
                right = right + jnp.dot(high[s], w, preferred_element_type=F32)
                right = right + jnp.dot(low[s], w, preferred_element_type=F32)
            for k in range(lanes // LANES):
                rows_ref[:, first + lane // LANES + k, :] = right[:, k * LANES : (k + 1) * LANES]
    zero = jnp.zeros((probes, LANES), F32)
    for k in range(plan.data, plan.high):
        rows_ref[:, k, :] = zero
    table = lane_table(squares, probes)
    high = table.astype(TAIL).astype(F32)
    rows_ref[:, plan.high, :] = high
    rows_ref[:, plan.low, :] = table - high


def split_again(plan, total, axis, dtype):
    row = lax.broadcasted_iota(jnp.int32, total.shape, axis)
    table = lax.slice_in_dim(total, plan.high, plan.high + 1, axis=axis)
    table = table + lax.slice_in_dim(total, plan.low, plan.low + 1, axis=axis)
    high = table.astype(dtype).astype(F32)
    return jnp.where(row == plan.high, high, jnp.where(row == plan.low, table - high, total))


def sum_parts(plan, in_ref, out_ref):
    dtype = out_ref.dtype
    out_ref[...] = split_again(plan, sum_of(in_ref), 1, dtype).astype(dtype)


def sum_copies(plan, in_ref, out_ref):
    dtype = out_ref.dtype
    total = split_again(plan, sum_of(in_ref), 0, dtype).astype(dtype)
    for j in range(plan.zs):
        out_ref[j] = total


def own_squares(plan, y_ref, out_ref):
    columns = []
    for first, n, _ in plan.part:
        y = y_ref[first : first + n, :]
        total = jnp.sum(y * y, axis=1, keepdims=True)
        columns.append(jnp.sum(total, axis=0, keepdims=True))
    table = lane_table(columns, out_ref.shape[1])
    for j in range(plan.cols):
        out_ref[j] = table


def unit(plan, stats_ref, y_ref, q_ref, out_ref):
    q = sum_of(q_ref)[:1]
    row = lax.broadcasted_iota(jnp.int32, stats_ref.shape[1:], 0)
    mine = row == lax.axis_index("z")
    s1, scale, square_scale = (
        jnp.sum(jnp.where(mine, stats_ref[k], 0.0), axis=0, keepdims=True) for k in range(3)
    )
    outs, _ = plan.part_counts(1)
    t2 = (y_ref[plan.high : plan.high + 1, :] + y_ref[plan.low : plan.low + 1, :]) / square_scale
    f2 = s1 * lax.rsqrt(s1 * s1 * t2 / outs + EPS)
    root = jnp.sqrt(q) / scale * f2
    table = jnp.log(jnp.maximum(root, 1e-37))
    out_ref[...] = jnp.zeros(out_ref.shape, F32)
    for i, (first, n, inp) in enumerate(plan.part):
        factor = lax.rsqrt(jnp.maximum(q[:, i : i + 1] / float(inp * plan.cols), 1e-30))
        out_ref[first : first + n, :] = y_ref[first : first + n, :] * factor
    high = table.astype(TAIL).astype(F32)
    out_ref[plan.high : plan.high + 1, :] = high
    out_ref[plan.low : plan.low + 1, :] = table - high


def finish(plan, v_ref, oa, ob, oc, sa, sb, sc):
    probes = v_ref.shape[2]
    outs, ins = plan.counts(probes)
    parts = [v_ref[x, plan.high].astype(F32) + v_ref[x, plan.low].astype(F32) for x in range(plan.xs)]
    root = jnp.exp(by_matrix(plan, parts))
    spread = root * lax.rsqrt(ins)
    scale = spread * lax.rsqrt(spread * spread + EPS)
    sigma = (root * lax.rsqrt(outs)).T
    m = 0
    for ref, sig in ((oa, sa), (ob, sb), (oc, sc)):
        n1, n2 = (ref.shape[0], 1) if ref.ndim == 3 else ref.shape[:2]
        if sig.ndim == 2:
            sig[...] = sigma[m : m + n1]
        else:
            for k in range(n1):
                sig[k] = sigma[m + k * n2 : m + (k + 1) * n2]
        for k in range(n1 * n2):
            part, first, _ = plan.where[m]
            for b in range(plan.ins[m] // LANES):
                value = v_ref[part, first + b].astype(F32) * scale[:, m : m + 1]
                here = slice(b * LANES, (b + 1) * LANES)
                if ref.ndim == 3:
                    ref[k, :, here] = value
                else:
                    ref[k // n2, k % n2, :, here] = value
            m += 1


def swap(v, axis):
    return lax.all_to_all(v, axis, 0, 0, tiled=True)


def steps(gate_up, down_weight, query_output, probe_gate, probe_down, probe_query):
    xs, zs, ys = lax.axis_size("x"), lax.axis_size("z"), lax.axis_size("y")
    cols = lax.axis_size(COL)
    weights = (gate_up, down_weight, query_output)
    vectors = (probe_gate, probe_down, probe_query)
    probes = probe_down.shape[1]
    plan = Plan(weights, xs, zs, cols)
    bind = lambda f, *rest: functools.partial(f, *rest)
    blocks = plan.blocks
    left_shape = sds((probes, plan.left_pad + LANES), F32)
    copies_shape = lambda n: sds((n, probes, plan.left_pad + 2 * LANES), BF16)
    rows = pltpu.VMEM((xs, probes, blocks, LANES), F32)

    def left_sums(left):
        cores = lax.axis_size("core")
        other = lax.ppermute(left, "core", [(i, (i + 1) % cores) for i in range(cores)])
        return call(bind(pair_sum, plan), copies_shape(ys), left, other)

    def by_block(copies):
        return jnp.swapaxes(swap(copies, "z"), 0, 1)

    held = [pltpu.VMEM(x.shape, x.dtype) for pair in zip(vectors, weights) for x in pair]
    strips = xs * sum(len(strips) for strips in plan.strips)
    left, *packs = call(
        bind(first_left, plan),
        (copies_shape(cols),) + (sds((plan.packed, plan.width), BF16),) * xs,
        *weights,
        *vectors,
        specs=[HBM] * 6,
        out_specs=(VMEM,) + (HBM,) * xs,
        scratch=[*held, pltpu.SemaphoreType.DMA((6,)), pltpu.SemaphoreType.DMA((strips,))],
        limit=FIRST,
    )
    left = swap(left, COL)
    for s in range(1, xs):
        packs[s] = lax.ppermute(packs[s], "x", [(i, (i + s) % xs) for i in range(xs)])
    shape = sds((xs, probes, blocks, LANES), BF16)
    right = call(bind(first_right, plan), shape, *weights, left, scratch=[rows])
    right = swap(right, "x")
    right = call(bind(sum_parts, plan), sds((probes, blocks, LANES), BF16), right)
    right = swap(right, "z")
    right = call(bind(sum_copies, plan), sds((zs, blocks, LANES), BF16), right)
    v1 = by_block(right)

    left = call(bind(next_left, plan), left_shape, *packs, v1)
    left = swap(left_sums(left), "y")
    shapes = (sds((probes, blocks, LANES), F32), sds((3, probes, LANES), F32))
    right, stats = call(bind(last_right, plan), shapes, *packs, left, v1)
    right = jnp.sum(swap(right.astype(WIRE), "z").astype(F32), axis=0)
    q2 = call(bind(own_squares, plan), sds((cols, 8, LANES), F32), right)
    q2 = swap(q2, COL)
    own = call(bind(unit, plan), sds((blocks, LANES), F32), stats, right, q2)
    part = by_block(jnp.broadcast_to(own.astype(WIRE)[None], (zs, *own.shape)))
    v2 = swap(jnp.broadcast_to(part[None], (xs, *part.shape)), "x").astype(F32)
    outs = tuple(sds(v.shape, F32) for v in vectors)
    outs += tuple(sds(v.shape[:-1], F32) for v in vectors)
    return call(bind(finish, plan), outs, v2)


def solution(mesh):
    cols = mesh.shape["col"]
    finer = Mesh(mesh.devices.reshape(16, -1, cols // 2, 2), ("z", "x", *COL))
    row = ("z", "x")
    in_specs = (
        P(None, None, row, COL),
        P(None, row, COL),
        P(None, None, row, COL),
        P(None, None, None, COL),
        P(None, None, COL),
        P(None, None, None, COL),
    )
    out_specs = (
        P(None, None, None, COL),
        P(None, None, COL),
        P(None, None, None, COL),
        P(),
        P(),
        P(),
    )
    return jax.shard_map(steps, mesh=finer, in_specs=in_specs, out_specs=out_specs, check_vma=False)
```
